256 devices in a mesh: sec: 16 (over y, x), pair: 16 (over z, core).
Axes of the slice: x: 4, y: 4, z: 8, core: 2. Of those that a mesh axis runs over, the one named last changes fastest.
Arguments:
- left_ops: bfloat16 [16, 528, 256, 256], P('sec', 'pair'), may hold values from -6 to 6
- rotation: bfloat16 [16, 256, 128], P('sec'), may hold values from -0.375 to 0.375
- integrals: bfloat16 [528, 528], replicated, may hold values from -0.25 to 0.25
- right_ops: bfloat16 [16, 528, 128, 128], P('sec', 'pair'), may hold values from -0.001953125 to 0.001953125
- states: bfloat16 [16, 16, 128, 128], P('sec', None, 'pair'), may hold values from -6 to 6
- sector_sizes: int32 [16], P('sec'), may hold values from 32 to 128, as said below
- couplings: int32 [16, 4], P('sec'), may hold values from -1 to 15, as said below
- pair_order: int32 [528], replicated, may hold values from 0 to 527, each once
Outputs:
- sigma: float32 [16, 16, 128, 128], P('sec', None, 'pair')
The draws below stay inside these ranges and needn't reach their ends.
Inputs may be any that keep to these rules, and one draw needn't show every extreme that they name: `sector_sizes`: some sector keeps all 128 states and some keeps 128 // 4. `couplings`: each row lists 1 to 4 distinct sectors in its first slots and -1 in the rest; some row is full and some lists one sector. `pair_order`: each pair appears once.
All inputs are finite; a program needn't handle non-finite values.
Results may differ from the reference program's by a relative error of at most 0.0064.
Values may be sent and summed in bfloat16 or wider, within the bound.
No kernel may reach another device: no remote copies, remote signals or barrier semaphores. Data moves between devices by JAX's collectives and lax.ppermute only.
A program may use at most 64 MiB of HBM per device.

```python
import jax
import jax.numpy as jnp
from jax import lax

B0 = 256
M = 128
MR = 128
P_SIZE = 528
ROOTS = 16
KMAX = 4
SECTORS = 16


def draw_sector_sizes(key, part):
    base = jax.random.fold_in(key, 11)
    first, second, third = jax.random.split(base, 3)
    sizes = jax.random.randint(first, (SECTORS,), M // 4, M + 1)
    top = jax.random.randint(second, (), 0, SECTORS)
    offset = jax.random.randint(third, (), 1, SECTORS)
    bottom = (top + offset) % SECTORS
    index = jnp.arange(SECTORS)
    sizes = jnp.where(index == top, M, sizes)
    sizes = jnp.where(index == bottom, M // 4, sizes)
    return sizes.astype(jnp.int32)


def draw_couplings(key, part):
    base = jax.random.fold_in(key, 23)
    first, second, third, fourth = jax.random.split(base, 4)
    counts = jax.random.randint(first, (SECTORS,), 1, KMAX + 1)
    full_row = jax.random.randint(second, (), 0, SECTORS)
    offset = jax.random.randint(third, (), 1, SECTORS)
    single_row = (full_row + offset) % SECTORS
    index = jnp.arange(SECTORS)
    counts = jnp.where(index == full_row, KMAX, counts)
    counts = jnp.where(index == single_row, 1, counts)
    row_keys = jax.random.split(fourth, SECTORS)
    orders = jax.vmap(lambda k: jax.random.permutation(k, SECTORS))(row_keys)[:, :KMAX]
    slots = jnp.arange(KMAX)[None, :]
    table = jnp.where(slots < counts[:, None], orders, -1)
    return table.astype(jnp.int32)


def level_of(key, shape, cuts, smallest, largest):
    factor_of = 1.0
    for dim, parts in cuts:
        draws = jax.random.uniform(jax.random.fold_in(jax.random.fold_in(key, 6), dim), (parts,), jnp.float32, smallest / len(cuts), largest / len(cuts))
        factor_of = factor_of * jnp.repeat(jnp.exp(draws), shape[dim] // parts).reshape((-1,) + (1,) * (len(shape) - 1 - dim))
    return factor_of


def normal_values(stream_key, dims, width, reach, cuts=(), kind=jnp.bfloat16):
    entries = width * jax.random.normal(stream_key, dims, jnp.float32)
    if cuts:
        entries = entries * level_of(stream_key, dims, cuts, -0.22, 0.18)
    return jnp.clip(entries, -reach, reach).astype(kind)


def setup_inputs(seed: int = 0) -> dict:
    streams_of = jax.random.split(jax.random.key(seed), 9)
    left_ops = normal_values(streams_of[0], (SECTORS, P_SIZE, B0, B0), 1.0, 6.0, ((0, 16), (1, 16)))
    rotation = normal_values(streams_of[1], (SECTORS, B0, M), B0 ** -0.5, 0.375, ((0, 16),))
    integrals = normal_values(streams_of[2], (P_SIZE, P_SIZE), P_SIZE ** -0.5, 0.25)
    right_ops = normal_values(streams_of[3], (SECTORS, P_SIZE, MR, MR), (M * MR * P_SIZE) ** -0.5, 0.001953125, ((0, 16), (1, 16)))
    states = normal_values(streams_of[4], (SECTORS, ROOTS, M, MR), 1.0, 6.0, ((0, 16), (2, 16)))
    sector_sizes = draw_sector_sizes(jax.random.fold_in(streams_of[8], 71), 0)
    couplings = draw_couplings(jax.random.fold_in(streams_of[8], 71), 0)
    pair_order = jax.random.permutation(streams_of[7], P_SIZE).astype(jnp.int32)
    return dict(left_ops=left_ops, rotation=rotation, integrals=integrals, right_ops=right_ops, states=states, sector_sizes=sector_sizes, couplings=couplings, pair_order=pair_order)


def reference(left_ops, rotation, integrals, right_ops, states, sector_sizes, couplings, pair_order):
    ordered = jnp.take(integrals, pair_order.astype(jnp.int32), axis=1).astype(jnp.float32)
    sector_ids = jnp.arange(SECTORS, dtype=jnp.int32)
    weights = jnp.sum((couplings[:, :, None] == sector_ids[None, None, :]).astype(jnp.float32), axis=1)
    mixed_all = jnp.einsum('st,trab->srab', weights, states.astype(jnp.float32)).astype(jnp.bfloat16)
    block = 48 if P_SIZE % 48 == 0 else P_SIZE
    count = P_SIZE // block

    def one_sector(items):
        ops, rot, size, rops, mixed = items
        live = jnp.arange(M, dtype=jnp.int32) < size
        kept = jnp.where(live[None, :], rot, jnp.zeros_like(rot))
        keptf = kept.astype(jnp.float32)
        half = jnp.einsum('pij,jk->pik', ops.astype(jnp.float32), keptf).astype(jnp.bfloat16)
        rotated = jnp.einsum('jm,pjk->pmk', keptf, half.astype(jnp.float32)).astype(jnp.bfloat16)
        complementary = jnp.einsum('qi,iab->qab', ordered, rotated.astype(jnp.float32)).astype(jnp.bfloat16)
        qblocks = complementary.reshape(count, block, M, M)
        rblocks = rops.reshape(count, block, MR, MR)
        mixedf = mixed.astype(jnp.float32)

        def accumulate(total, pieces):
            qpiece, rpiece = pieces
            image = jnp.einsum('rbd,qcd->qrbc', mixedf, rpiece.astype(jnp.float32)).astype(jnp.bfloat16)
            total = total + jnp.einsum('qab,qrbc->rac', qpiece.astype(jnp.float32), image.astype(jnp.float32))
            return total, None

        start = jnp.zeros((ROOTS, M, MR), jnp.float32)
        total, _ = lax.scan(accumulate, start, (qblocks, rblocks))
        return total

    return lax.map(one_sector, (left_ops, rotation, sector_sizes, right_ops, mixed_all))
```

```python
import jax
import jax.numpy as jnp
from jax import lax
from jax.sharding import Mesh
from jax.sharding import PartitionSpec as P


SEC = ("y", "x")
PAIR = ("z", "core")
FAR_FIRST = (4, 3, -3, 2, -2, 1, -1)


def other_core(x):
    return lax.ppermute(x, "core", [(0, 1), (1, 0)])


def cores_in_order(own, other, dim):
    first = lax.axis_index("core") == 0
    return jnp.where(
        first, jnp.stack([own, other], axis=dim), jnp.stack([other, own], axis=dim)
    )


def exchange_over_z(blocks):
    n = lax.axis_size("z")
    me = lax.axis_index("z")
    arrived = []
    for shift in FAR_FIRST:
        block = lax.dynamic_index_in_dim(blocks, (me + shift) % n, 0, keepdims=False)
        pairs = [(i, (i + shift) % n) for i in range(n)]
        arrived.append((shift, lax.ppermute(block, "z", pairs)))
    own = lax.dynamic_index_in_dim(blocks, me, 0)
    whole = lax.dynamic_update_slice_in_dim(jnp.zeros_like(blocks), own, me, 0)
    for shift, block in arrived:
        whole = lax.dynamic_update_slice_in_dim(whole, block[None], (me - shift) % n, 0)
    return whole


def local(left_ops, rotation, integrals, right_ops, states, sector_sizes, couplings, pair_order):
    core = lax.axis_index("core")
    zs = lax.axis_size("z")
    cores = lax.axis_size("core")
    width = rotation.shape[2]
    pairs = left_ops.shape[1]
    roots, rows = states.shape[1], states.shape[2]
    sectors = lax.axis_size(SEC)

    sources = lax.all_to_all(
        jnp.broadcast_to(states, (sectors, *states.shape[1:])), SEC, 0, 0, tiled=True
    )

    live = jnp.arange(width, dtype=jnp.int32) < sector_sizes[0]
    kept = jnp.where(live[None, :], rotation[0], jnp.zeros_like(rotation[0]))
    slot = jnp.arange(width, dtype=jnp.int32)
    which, rest = slot // (zs * rows), slot % (zs * rows)
    column = (rest // rows) * (cores * rows) + jnp.where(which == 0, core, 1 - core) * rows + rest % rows
    pick = (slot[:, None] == column[None, :]).astype(jnp.bfloat16)
    kept_rows = jnp.dot(kept, pick, preferred_element_type=jnp.float32).astype(jnp.bfloat16)

    half = jnp.einsum("pij,jk->pik", left_ops[0], kept, preferred_element_type=jnp.float32).astype(
        jnp.bfloat16
    )
    rotated = jnp.einsum("jm,pjk->pmk", kept_rows, half, preferred_element_type=jnp.float32).astype(
        jnp.bfloat16
    )
    rotated = rotated.reshape(pairs, cores, zs, rows, width).transpose(1, 2, 0, 3, 4)
    rotated = cores_in_order(rotated[0], other_core(rotated[1]), 1)
    rotated = rotated.reshape(zs, cores * pairs, rows, width)
    rotated_all = exchange_over_z(rotated).reshape(zs * cores * pairs, rows, width)

    all_pairs = integrals.shape[1]
    taken = (jnp.arange(all_pairs, dtype=jnp.int32)[:, None] == pair_order[None, :]).astype(jnp.bfloat16)
    ordered = jnp.dot(integrals, taken, preferred_element_type=jnp.float32).astype(jnp.bfloat16)

    sector_ids = jnp.arange(sectors, dtype=jnp.int32)
    weights = jnp.sum(
        (couplings[0][:, None] == sector_ids[None, :]).astype(jnp.float32), axis=0
    )
    mixed_rows = jnp.sum(
        weights[:, None, None, None] * sources.astype(jnp.float32), axis=0
    ).astype(jnp.bfloat16)
    mixed_z = lax.all_to_all(
        jnp.broadcast_to(mixed_rows[None], (zs, *mixed_rows.shape)), "z", 0, 0, tiled=True
    )
    mixed = cores_in_order(mixed_z, other_core(mixed_z), 1)
    mixed = mixed.transpose(2, 0, 1, 3, 4).reshape(roots, width, width)

    image = jnp.einsum(
        "rbd,qcd->qrbc", mixed, right_ops[0], preferred_element_type=jnp.float32
    ).astype(jnp.bfloat16)

    comp = jnp.einsum(
        "qi,iab->qab", ordered, rotated_all, preferred_element_type=jnp.float32
    ).astype(jnp.bfloat16)
    comp = exchange_over_z(comp.reshape(zs, cores * pairs, rows, width))
    comp = comp.reshape(zs, cores, pairs, rows, width)
    own = lax.dynamic_index_in_dim(comp, core, 1, keepdims=False)
    theirs = lax.dynamic_index_in_dim(comp, 1 - core, 1, keepdims=False)
    comp = cores_in_order(own, other_core(theirs), 1)
    comp = comp.transpose(2, 0, 1, 3, 4).reshape(pairs, width, width)

    total = jnp.einsum("qab,qrbc->rac", comp, image, preferred_element_type=jnp.float32)
    total = total.reshape(roots, zs, cores, rows, width)
    own = lax.dynamic_index_in_dim(total, core, 2, keepdims=False)
    theirs = lax.dynamic_index_in_dim(total, 1 - core, 2, keepdims=False)
    chip = own + other_core(theirs.astype(jnp.bfloat16)).astype(jnp.float32)
    parts = chip.astype(jnp.bfloat16).transpose(1, 0, 2, 3)
    parts = lax.all_to_all(parts, "z", 0, 0, tiled=True)
    return parts.astype(jnp.float32).sum(axis=0)[None]


def solution(mesh):
    torus = Mesh(mesh.devices.reshape(4, 4, -1, 2), ("y", "x", "z", "core"))
    placed = (
        P(SEC, PAIR, None, None),
        P(SEC, None, None),
        P(),
        P(SEC, PAIR, None, None),
        P(SEC, None, PAIR, None),
        P(SEC),
        P(SEC, None),
        P(),
    )
    return jax.shard_map(
        local, mesh=torus, in_specs=placed, out_specs=P(SEC, None, PAIR, None), check_vma=False
    )
```

```python
import functools

import jax
import jax.numpy as jnp
from jax import lax
from jax.experimental import pallas as pl
from jax.experimental.pallas import tpu as pltpu
from jax.sharding import Mesh
from jax.sharding import PartitionSpec as P


SEC = ("y", "x")
PAIR = ("z", "core")
FAR_FIRST = (4, 3, -3, 2, -2, 1, -1)
F32 = jnp.float32
BF16 = jnp.bfloat16
VMEM = pl.BlockSpec(memory_space=pltpu.VMEM)


def dot(a, b, dims):
    return lax.dot_general(a, b, (dims, ((), ())), preferred_element_type=F32)


def rotate_kernel(group, zs, rows, scalars, left, rotation, own, other, kept_ref, rows_ref):
    size, core = scalars[0], scalars[1]
    depth, width = rotation.shape

    @pl.when(pl.program_id(0) == 0)
    def _():
        live = lax.broadcasted_iota(jnp.int32, (depth, width), 1) < size
        kept = jnp.where(live, rotation[...].astype(F32), 0.0).astype(BF16)
        kept_ref[...] = kept
        slot = lax.broadcasted_iota(jnp.int32, (width, width), 0)
        target = lax.broadcasted_iota(jnp.int32, (width, width), 1)
        half = zs * rows
        which = (slot >= half).astype(jnp.int32)
        rest = slot - which * half
        place = core + which - 2 * core * which
        chip = lax.shift_right_logical(rest, 3)
        column = chip * (2 * rows) + place * rows + (rest - chip * rows)
        pick = jnp.where(column == target, 1.0, 0.0).astype(BF16)
        rows_ref[...] = dot(pick, kept, ((1,), (1,))).astype(BF16)

    kept = kept_ref[...]
    mine = rows_ref[...]
    flat = left[...].reshape(group * depth, depth)
    half = dot(flat, kept, ((1,), (0,))).astype(BF16)
    for g in range(group):
        result = dot(mine, half[g * depth : (g + 1) * depth], ((1,), (0,)))
        for chip in range(zs):
            own[chip, g] = result[chip * rows : (chip + 1) * rows].astype(BF16)
            low = (zs + chip) * rows
            other[chip, g] = result[low : low + rows].astype(BF16)


def rotate(left, rotation, scalars, zs, rows, group):
    pairs, depth, _ = left.shape
    width = rotation.shape[1]
    shape = jax.ShapeDtypeStruct((zs, pairs, rows, width), BF16)
    block = pl.BlockSpec((zs, group, rows, width), lambda g: (0, g, 0, 0))
    return pl.pallas_call(
        functools.partial(rotate_kernel, group, zs, rows),
        grid=(pairs // group,),
        in_specs=[
            pl.BlockSpec(memory_space=pltpu.SMEM),
            pl.BlockSpec((group, depth, depth), lambda g: (g, 0, 0)),
            pl.BlockSpec((depth, width), lambda g: (0, 0)),
        ],
        out_specs=[block, block],
        out_shape=[shape, shape],
        scratch_shapes=[pltpu.VMEM((depth, width), BF16), pltpu.VMEM((width, depth), BF16)],
    )(scalars, left, rotation)


def image_kernel(chunk, mixed, right, image):
    roots, width, _ = mixed.shape
    pairs = right.shape[0]

    def put(first, count):
        ops = right[pl.ds(first, count)].reshape(count * width, width)
        for start in range(0, roots, chunk):
            block = mixed[start : start + chunk].reshape(chunk * width, width)
            result = dot(block, ops, ((1,), (1,))).astype(BF16)
            for r in range(chunk):
                for j in range(count):
                    image[
                        pl.ds(pl.multiple_of((first + j) * width, width), width),
                        (start + r) * width : (start + r + 1) * width,
                    ] = result[r * width : (r + 1) * width, j * width : (j + 1) * width]

    def step(i, carry):
        put(2 * i, 2)
        return carry

    lax.fori_loop(0, pairs // 2, step, 0)
    if pairs % 2:
        put(pairs - 1, 1)


def make_image(mixed, right):
    roots, width, _ = mixed.shape
    pairs = right.shape[0]
    return pl.pallas_call(
        functools.partial(image_kernel, 4),
        in_specs=[VMEM, VMEM],
        out_specs=VMEM,
        out_shape=jax.ShapeDtypeStruct((pairs * width, roots * width), BF16),
    )(mixed, right)


def sigma_kernel(comp, image, total):
    pairs, width, _ = comp.shape
    tile = 256

    def step(n, carry):
        lanes = pl.ds(pl.multiple_of(n * tile, tile), tile)
        sums = jnp.zeros((width, tile), F32)
        for q in range(0, pairs - 1, 2):
            two = jnp.concatenate([comp[q], comp[q + 1]], axis=1)
            sums += dot(two, image[q * width : (q + 2) * width, lanes], ((1,), (0,)))
        if pairs % 2:
            sums += dot(comp[pairs - 1], image[(pairs - 1) * width : pairs * width, lanes], ((1,), (0,)))
        total[:, lanes] = sums
        return carry

    lax.fori_loop(0, image.shape[1] // tile, step, 0)


def make_sigma(comp, image):
    return pl.pallas_call(
        sigma_kernel,
        in_specs=[VMEM, VMEM],
        out_specs=VMEM,
        out_shape=jax.ShapeDtypeStruct((comp.shape[1], image.shape[1]), F32),
    )(comp, image)


def other_core(x):
    return lax.ppermute(x, "core", [(0, 1), (1, 0)])


def in_core_order(own, other, dim):
    first = lax.axis_index("core") == 0
    return jnp.where(
        first, jnp.stack([own, other], axis=dim), jnp.stack([other, own], axis=dim)
    )


def send_over_z(block_of):
    n = lax.axis_size("z")
    me = lax.axis_index("z")
    arrived = []
    for shift in FAR_FIRST:
        pairs = [(i, (i + shift) % n) for i in range(n)]
        block = block_of(lax.rem(me + (shift + n), n))
        arrived.append(lax.ppermute(block, "z", pairs))
    return arrived


def place_by_source(own, arrived):
    n = lax.axis_size("z")
    me = lax.axis_index("z")
    whole = lax.dynamic_update_slice_in_dim(jnp.zeros((n, *own.shape), own.dtype), own[None], me, 0)
    for shift, block in zip(FAR_FIRST, arrived):
        whole = lax.dynamic_update_slice_in_dim(whole, block[None], lax.rem(me + (n - shift), n), 0)
    return whole


def body(left_ops, rotation, integrals, right_ops, states, sector_sizes, couplings, pair_order):
    core = lax.axis_index("core")
    zs = lax.axis_size("z")
    cores = lax.axis_size("core")
    me = lax.axis_index("z")
    width = rotation.shape[2]
    pairs = left_ops.shape[1]
    roots, rows = states.shape[1], states.shape[2]
    sectors = lax.axis_size(SEC)
    all_pairs = integrals.shape[1]

    def flip(x):
        parts = x.reshape(zs, cores, pairs, *x.shape[1:])
        return jnp.where(core == 0, parts, parts[:, ::-1]).reshape(x.shape)

    scalars = jnp.stack([sector_sizes[0], core.astype(jnp.int32)])
    own, other = rotate(left_ops[0], rotation[0], scalars, zs, rows, 3)
    theirs = other_core(other)

    copies = jnp.broadcast_to(states, (sectors, *states.shape[1:]))
    sources = lax.all_to_all(copies, SEC, 0, 0, tiled=True)

    def rotated_block(chip):
        return jnp.concatenate(
            [
                lax.dynamic_index_in_dim(own, chip, 0, keepdims=False),
                lax.dynamic_index_in_dim(theirs, chip, 0, keepdims=False),
            ],
            axis=0,
        )

    arrived = send_over_z(rotated_block)
    rotated_all = place_by_source(rotated_block(me), arrived)
    rotated_all = rotated_all.reshape(all_pairs, rows, width)

    order = flip(pair_order)
    taken = (jnp.arange(all_pairs, dtype=jnp.int32)[:, None] == order[None, :]).astype(BF16)
    ordered = jnp.dot(flip(integrals), taken, preferred_element_type=F32).astype(BF16)
    ordered, rotated_all = lax.optimization_barrier((ordered, rotated_all))

    sector_ids = jnp.arange(sectors, dtype=jnp.int32)
    weights = jnp.sum((couplings[0][:, None] == sector_ids[None, :]).astype(F32), axis=0)
    mixed_rows = jnp.sum(
        weights[:, None, None, None] * sources.astype(F32), axis=0
    ).astype(BF16)
    copies = jnp.broadcast_to(mixed_rows[None], (zs, *mixed_rows.shape))
    mixed_z = lax.all_to_all(copies, "z", 0, 0, tiled=True)
    mixed_other = other_core(mixed_z)
    mixed = in_core_order(mixed_z, mixed_other, 1)
    mixed = mixed.transpose(2, 0, 1, 3, 4).reshape(roots, width, width)
    image = make_image(mixed, right_ops[0])

    comp = jnp.einsum("qi,iab->qab", ordered, rotated_all, preferred_element_type=F32).astype(BF16)
    comp = comp.reshape(zs, cores * pairs, rows, width)

    def comp_block(chip):
        return lax.dynamic_index_in_dim(comp, chip, 0, keepdims=False)

    arrived = send_over_z(comp_block)
    blocks = [comp_block(me)] + arrived
    mine = jnp.stack([b[:pairs] for b in blocks], axis=1)
    theirs = other_core(jnp.stack([b[pairs:] for b in blocks], axis=1))
    comp = jnp.concatenate([mine, theirs], axis=1).reshape(pairs, width, width)

    total = make_sigma(comp, image)
    total = total.reshape(cores, zs, rows, roots * width)
    theirs = other_core(total[1].astype(BF16))
    chip = (total[0] + theirs.astype(F32)).astype(BF16)

    place = {shift % zs: number + 1 for number, shift in enumerate(FAR_FIRST)}
    place[0] = 0
    by_shift = jnp.stack([chip[place[s]] for s in range(zs)])
    twice = jnp.concatenate([by_shift[::-1], by_shift[::-1]], axis=0)
    parts = lax.dynamic_slice_in_dim(twice, zs - 1 - me, zs, 0)
    parts = lax.all_to_all(parts, "z", 0, 0, tiled=True)
    result = parts.astype(F32).sum(axis=0)
    return result.reshape(rows, roots, width).transpose(1, 0, 2)[None]


def solution(mesh):
    torus = Mesh(mesh.devices.reshape(4, 4, -1, 2), ("y", "x", "z", "core"))
    placed = (
        P(SEC, PAIR, None, None),
        P(SEC, None, None),
        P(),
        P(SEC, PAIR, None, None),
        P(SEC, None, PAIR, None),
        P(SEC),
        P(SEC, None),
        P(),
    )
    return jax.shard_map(
        body, mesh=torus, in_specs=placed, out_specs=P(SEC, None, PAIR, None), check_vma=False
    )
```

```python
import functools

import jax
import jax.numpy as jnp
from jax import lax
from jax.experimental import pallas as pl
from jax.experimental.pallas import tpu as pltpu
from jax.sharding import Mesh
from jax.sharding import PartitionSpec as P


SEC = ("y", "x")
PAIR = ("z", "core")
FAR_FIRST = (4, 3, -3, 2, -2, 1, -1)
F32 = jnp.float32
BF16 = jnp.bfloat16
VMEM = pl.BlockSpec(memory_space=pltpu.VMEM)


def grant(mib):
    return pltpu.CompilerParams(vmem_limit_bytes=mib * 1024 * 1024)


def dot(a, b, dims):
    return lax.dot_general(a, b, (dims, ((), ())), preferred_element_type=F32)


def rotate_kernel(group, zs, rows, scalars, left, rotation, own, other, kept_ref, rows_ref):
    size, core = scalars[0], scalars[1]
    depth, width = rotation.shape

    @pl.when(pl.program_id(0) == 0)
    def _():
        live = lax.broadcasted_iota(jnp.int32, (depth, width), 1) < size
        kept = jnp.where(live, rotation[...].astype(F32), 0.0).astype(BF16)
        kept_ref[...] = kept
        slot = lax.broadcasted_iota(jnp.int32, (width, width), 0)
        target = lax.broadcasted_iota(jnp.int32, (width, width), 1)
        half = zs * rows
        which = (slot >= half).astype(jnp.int32)
        rest = slot - which * half
        place = core + which - 2 * core * which
        chip = lax.shift_right_logical(rest, 3)
        column = chip * (2 * rows) + place * rows + (rest - chip * rows)
        pick = jnp.where(column == target, 1.0, 0.0).astype(BF16)
        rows_ref[...] = dot(pick, kept, ((1,), (1,))).astype(BF16)

    kept = kept_ref[...]
    mine = rows_ref[...]
    parts = [dot(mine, left[g], ((1,), (0,))).astype(BF16) for g in range(group)]
    whole = dot(jnp.concatenate(parts, axis=0), kept, ((1,), (0,))).astype(BF16)
    for g in range(group):
        result = whole[g * width : (g + 1) * width].reshape(2, zs, rows, width)
        own[:, g] = result[0]
        other[:, g] = result[1]


def rotate(left, rotation, scalars, zs, rows, group):
    pairs, depth, _ = left.shape
    width = rotation.shape[1]
    shape = jax.ShapeDtypeStruct((zs, pairs, rows, width), BF16)
    block = pl.BlockSpec((zs, group, rows, width), lambda g: (0, g, 0, 0))
    return pl.pallas_call(
        functools.partial(rotate_kernel, group, zs, rows),
        grid=(pairs // group,),
        in_specs=[
            pl.BlockSpec(memory_space=pltpu.SMEM),
            pl.BlockSpec((group, depth, depth), lambda g: (g, 0, 0)),
            pl.BlockSpec((depth, width), lambda g: (0, 0)),
        ],
        out_specs=[block, block],
        out_shape=[shape, shape],
        scratch_shapes=[pltpu.VMEM((depth, width), BF16), pltpu.VMEM((width, depth), BF16)],
        compiler_params=grant(10),
    )(scalars, left, rotation)


def image_kernel(chunk, mixed, right, image):
    roots, width, _ = mixed.shape
    pairs = right.shape[0]

    def put(first, count):
        ops = right[pl.ds(first, count)].reshape(count * width, width)
        for start in range(0, roots, chunk):
            block = mixed[start : start + chunk].reshape(chunk * width, width)
            result = dot(block, ops, ((1,), (1,))).astype(BF16)
            for r in range(chunk):
                for j in range(count):
                    image[
                        pl.ds(pl.multiple_of((first + j) * width, width), width),
                        (start + r) * width : (start + r + 1) * width,
                    ] = result[r * width : (r + 1) * width, j * width : (j + 1) * width]

    def step(i, carry):
        put(4 * i, 2)
        put(4 * i + 2, 2)
        return carry

    lax.fori_loop(0, pairs // 4, step, 0)
    for first in range(pairs - pairs % 4, pairs):
        put(first, 1)


def make_image(mixed, right):
    roots, width, _ = mixed.shape
    pairs = right.shape[0]
    return pl.pallas_call(
        functools.partial(image_kernel, 4),
        in_specs=[VMEM, VMEM],
        out_specs=VMEM,
        out_shape=pltpu.VMEM((pairs * width, roots * width), BF16),
        compiler_params=grant(5),
    )(mixed, right)


def sigma_kernel(comp, image, own, other):
    pairs, width, _ = comp.shape
    half = own.shape[0]
    sums = jnp.zeros((width, image.shape[1]), F32)
    for q in range(0, pairs - 1, 2):
        two = jnp.concatenate([comp[q], comp[q + 1]], axis=1)
        sums += dot(two, image[q * width : (q + 2) * width], ((1,), (0,)))
    if pairs % 2:
        sums += dot(comp[pairs - 1], image[(pairs - 1) * width : pairs * width], ((1,), (0,)))
    own[...] = sums[:half]
    other[...] = sums[half:].astype(BF16)


def make_sigma(comp, image):
    half = comp.shape[1] // 2
    return pl.pallas_call(
        sigma_kernel,
        in_specs=[VMEM, VMEM],
        out_specs=[VMEM, VMEM],
        out_shape=[
            pltpu.VMEM((half, image.shape[1]), F32),
            pltpu.VMEM((half, image.shape[1]), BF16),
        ],
        compiler_params=grant(8),
    )(comp, image)


def join_kernel(shifts, zs, scalars, own, theirs, *blocks):
    pairs = own.shape[1]
    for shift, block in zip(shifts, blocks):
        chip = lax.rem(scalars[0] + shift + zs, zs)
        block[:pairs] = own[chip]
        block[pairs:] = theirs[chip]


def cut_kernel(shifts, zs, scalars, whole, *blocks):
    for shift, block in zip(shifts, blocks):
        block[...] = whole[lax.rem(scalars[0] + shift + zs, zs)]


def split_kernel(shifts, zs, scalars, *refs):
    blocks, (mine, theirs) = refs[:-2], refs[-2:]
    pairs = mine.shape[1]
    core = scalars[1]
    for shift, block in zip(shifts, blocks):
        chip = lax.rem(scalars[0] - shift + zs, zs)
        mine[chip] = block[pl.ds(core * pairs, pairs)]
        theirs[chip] = block[pl.ds((1 - core) * pairs, pairs)]


def gather_kernel(shifts, zs, scalars, *refs):
    blocks, whole = refs[:-1], refs[-1]
    for shift, block in zip(shifts, blocks):
        whole[lax.rem(scalars[0] - shift + zs, zs)] = block[...]


def move(kernel, scalars, arrays, shapes, mib):
    shifts = (0,) + FAR_FIRST
    return pl.pallas_call(
        functools.partial(kernel, shifts, lax.axis_size("z")),
        in_specs=[pl.BlockSpec(memory_space=pltpu.SMEM)] + [VMEM] * len(arrays),
        out_specs=[VMEM] * len(shapes),
        out_shape=[pltpu.VMEM(shape, BF16) for shape in shapes],
        compiler_params=grant(mib),
    )(scalars, *arrays)


def other_core(x):
    return lax.ppermute(x, "core", [(0, 1), (1, 0)])


def in_core_order(own, other, dim):
    first = lax.axis_index("core") == 0
    return jnp.where(
        first, jnp.stack([own, other], axis=dim), jnp.stack([other, own], axis=dim)
    )


def send_over_z(blocks):
    n = lax.axis_size("z")
    arrived = []
    for shift, block in zip(FAR_FIRST, blocks):
        pairs = [(i, (i + shift) % n) for i in range(n)]
        arrived.append(lax.ppermute(block, "z", pairs))
    return arrived


def body(left_ops, rotation, integrals, right_ops, states, sector_sizes, couplings, pair_order):
    core = lax.axis_index("core")
    zs = lax.axis_size("z")
    cores = lax.axis_size("core")
    me = lax.axis_index("z")
    width = rotation.shape[2]
    pairs = left_ops.shape[1]
    roots, rows = states.shape[1], states.shape[2]
    sectors = lax.axis_size(SEC)
    all_pairs = integrals.shape[1]

    def flip(x):
        parts = x.reshape(zs, cores, pairs, *x.shape[1:])
        return jnp.where(core == 0, parts, parts[:, ::-1]).reshape(x.shape)

    left = pltpu.with_memory_space_constraint(left_ops[0], pltpu.HBM)
    turn = pltpu.with_memory_space_constraint(rotation[0], pltpu.HBM)
    scalars = jnp.stack([sector_sizes[0], core.astype(jnp.int32)])
    own, other = rotate(left, turn, scalars, zs, rows, 11)
    theirs = other_core(other)

    copies = jnp.broadcast_to(states, (sectors, *states.shape[1:]))
    sources = lax.all_to_all(copies, SEC, 0, 0, tiled=True)

    place = jnp.stack([me, core]).astype(jnp.int32)
    message = (cores * pairs, rows, width)
    blocks = move(join_kernel, place, (own, theirs), [message] * zs, 4)
    arrived = send_over_z(blocks[1:])
    arrived = [pltpu.with_memory_space_constraint(block, pltpu.VMEM) for block in arrived]
    (rotated_all,) = move(gather_kernel, place, [blocks[0]] + arrived, [(zs, *message)], 4)
    rotated_all = rotated_all.reshape(all_pairs, rows, width)

    order = flip(pair_order)
    taken = (jnp.arange(all_pairs, dtype=jnp.int32)[:, None] == order[None, :]).astype(BF16)
    ordered = jnp.dot(integrals, taken, preferred_element_type=F32).astype(BF16)
    ordered, rotated_all = lax.optimization_barrier((ordered, rotated_all))

    sector_ids = jnp.arange(sectors, dtype=jnp.int32)
    weights = jnp.sum((couplings[0][:, None] == sector_ids[None, :]).astype(F32), axis=0)
    mixed_rows = jnp.sum(weights[:, None, None, None] * sources.astype(F32), axis=0).astype(BF16)
    copies = jnp.broadcast_to(mixed_rows[None], (zs, *mixed_rows.shape))
    mixed_z = lax.all_to_all(copies, "z", 0, 0, tiled=True)
    mixed_other = other_core(mixed_z)
    mixed = in_core_order(mixed_z, mixed_other, 1)
    mixed = mixed.transpose(2, 0, 1, 3, 4).reshape(roots, width, width)
    image = make_image(mixed, right_ops[0])

    comp = jnp.einsum("qi,iab->qab", ordered, rotated_all, preferred_element_type=F32)
    comp = comp.astype(BF16)
    comp = comp.reshape(zs, cores * pairs, rows, width)

    blocks = move(cut_kernel, place, (comp,), [message] * zs, 4)
    arrived = send_over_z(blocks[1:])
    arrived = [pltpu.with_memory_space_constraint(block, pltpu.VMEM) for block in arrived]
    half = (zs, pairs, rows, width)
    mine, theirs = move(split_kernel, place, [blocks[0]] + arrived, [half] * 2, 4)
    theirs = other_core(theirs)
    comp = jnp.stack([mine, theirs]).transpose(2, 0, 1, 3, 4)
    comp = comp.reshape(pairs, width, width)

    total, given = make_sigma(comp, image)
    theirs = other_core(given)
    parts = (total + theirs.astype(F32)).astype(BF16).reshape(zs, rows, roots * width)
    parts = lax.all_to_all(parts, "z", 0, 0, tiled=True)
    result = parts.astype(F32).sum(axis=0)
    return result.reshape(rows, roots, width).transpose(1, 0, 2)[None]


def solution(mesh):
    torus = Mesh(mesh.devices.reshape(4, 4, -1, 2), ("y", "x", "z", "core"))
    placed = (
        P(SEC, PAIR, None, None),
        P(SEC, None, None),
        P(),
        P(SEC, PAIR, None, None),
        P(SEC, None, PAIR, None),
        P(SEC),
        P(SEC, None),
        P(),
    )
    return jax.shard_map(
        body, mesh=torus, in_specs=placed, out_specs=P(SEC, None, PAIR, None), check_vma=False
    )
```

```python
import functools

import jax
import jax.numpy as jnp
from jax import lax
from jax.experimental import pallas as pl
from jax.experimental.pallas import tpu as pltpu
from jax.sharding import Mesh
from jax.sharding import PartitionSpec as P


SEC = ("y", "x")
PAIR = ("z", "core")
FAR_FIRST = (4, 3, -3, 2, -2, 1, -1)
F32 = jnp.float32
BF16 = jnp.bfloat16
VMEM = pl.BlockSpec(memory_space=pltpu.VMEM)


def grant(mib):
    return pltpu.CompilerParams(vmem_limit_bytes=mib * 1024 * 1024)


def dot(a, b, dims):
    return lax.dot_general(a, b, (dims, ((), ())), preferred_element_type=F32)


def rotate_kernel(group, zs, rows, scalars, left, rotation, own, other, kept_ref, rows_ref):
    size, core = scalars[0], scalars[1]
    depth, width = rotation.shape

    @pl.when(pl.program_id(0) == 0)
    def _():
        live = lax.broadcasted_iota(jnp.int32, (depth, width), 1) < size
        kept = jnp.where(live, rotation[...].astype(F32), 0.0).astype(BF16)
        kept_ref[...] = kept
        slot = lax.broadcasted_iota(jnp.int32, (width, width), 0)
        target = lax.broadcasted_iota(jnp.int32, (width, width), 1)
        half = zs * rows
        which = (slot >= half).astype(jnp.int32)
        rest = slot - which * half
        place = core + which - 2 * core * which
        chip = lax.shift_right_logical(rest, 3)
        column = chip * (2 * rows) + place * rows + (rest - chip * rows)
        pick = jnp.where(column == target, 1.0, 0.0).astype(BF16)
        rows_ref[...] = dot(pick, kept, ((1,), (1,))).astype(BF16)

    kept = kept_ref[...]
    mine = rows_ref[...]
    parts = [dot(mine, left[g], ((1,), (0,))).astype(BF16) for g in range(group)]
    whole = dot(jnp.concatenate(parts, axis=0), kept, ((1,), (0,))).astype(BF16)
    for g in range(group):
        result = whole[g * width : (g + 1) * width].reshape(2, zs, rows, width)
        own[:, g] = result[0]
        other[:, g] = result[1]


def rotate(left, rotation, scalars, zs, rows, group):
    pairs, depth, _ = left.shape
    width = rotation.shape[1]
    shape = jax.ShapeDtypeStruct((zs, pairs, rows, width), BF16)
    block = pl.BlockSpec((zs, group, rows, width), lambda g: (0, g, 0, 0))
    return pl.pallas_call(
        functools.partial(rotate_kernel, group, zs, rows),
        grid=(pairs // group,),
        in_specs=[
            pl.BlockSpec(memory_space=pltpu.SMEM),
            pl.BlockSpec((group, depth, depth), lambda g: (g, 0, 0)),
            pl.BlockSpec((depth, width), lambda g: (0, 0)),
        ],
        out_specs=[block, block],
        out_shape=[shape, shape],
        scratch_shapes=[pltpu.VMEM((depth, width), BF16), pltpu.VMEM((width, depth), BF16)],
        compiler_params=grant(10),
    )(scalars, left, rotation)


def image_kernel(chunk, scalars, mine, theirs, right, image, placed, mixed):
    zs, roots, _, width = mine.shape
    pairs = right.shape[0]
    core = scalars[1]
    for chip in range(zs):
        placed[:, chip, core] = mine[chip]
        placed[:, chip, 1 - core] = theirs[chip]
    for root in range(roots):
        mixed[root] = placed[root].reshape(width, width)

    def put(first, count):
        ops = right[pl.ds(first, count)].reshape(count * width, width)
        for start in range(0, roots, chunk):
            block = mixed[start : start + chunk].reshape(chunk * width, width)
            result = dot(block, ops, ((1,), (1,))).astype(BF16)
            for r in range(chunk):
                for j in range(count):
                    image[
                        pl.ds(pl.multiple_of((first + j) * width, width), width),
                        (start + r) * width : (start + r + 1) * width,
                    ] = result[r * width : (r + 1) * width, j * width : (j + 1) * width]

    def step(i, carry):
        put(4 * i, 2)
        put(4 * i + 2, 2)
        return carry

    lax.fori_loop(0, pairs // 4, step, 0)
    for first in range(pairs - pairs % 4, pairs):
        put(first, 1)


def make_image(scalars, mine, theirs, right):
    zs, roots, rows, width = mine.shape
    pairs = right.shape[0]
    return pl.pallas_call(
        functools.partial(image_kernel, 4),
        in_specs=[pl.BlockSpec(memory_space=pltpu.SMEM), VMEM, VMEM, VMEM],
        out_specs=VMEM,
        out_shape=pltpu.VMEM((pairs * width, roots * width), BF16),
        scratch_shapes=[
            pltpu.VMEM((roots, zs, width // (zs * rows), rows, width), BF16),
            pltpu.VMEM((roots, width, width), BF16),
        ],
        compiler_params=grant(6),
    )(scalars, mine, theirs, right)


def sigma_kernel(mine, theirs, image, own, other):
    pairs, width = mine.shape[1], mine.shape[3]
    half = own.shape[0]
    comp = [
        jnp.concatenate([part[:, q].reshape(half, width) for part in (mine, theirs)], axis=0)
        for q in range(pairs)
    ]
    sums = jnp.zeros((width, image.shape[1]), F32)
    for q in range(0, pairs - 1, 2):
        two = jnp.concatenate([comp[q], comp[q + 1]], axis=1)
        sums += dot(two, image[q * width : (q + 2) * width], ((1,), (0,)))
    if pairs % 2:
        sums += dot(comp[pairs - 1], image[(pairs - 1) * width : pairs * width], ((1,), (0,)))
    own[...] = sums[:half]
    other[...] = sums[half:].astype(BF16)


def make_sigma(mine, theirs, image):
    half = mine.shape[0] * mine.shape[2]
    return pl.pallas_call(
        sigma_kernel,
        in_specs=[VMEM, VMEM, VMEM],
        out_specs=[VMEM, VMEM],
        out_shape=[
            pltpu.VMEM((half, image.shape[1]), F32),
            pltpu.VMEM((half, image.shape[1]), BF16),
        ],
        compiler_params=grant(8),
    )(mine, theirs, image)


def join_kernel(shifts, zs, scalars, own, theirs, *blocks):
    pairs = own.shape[1]
    core = scalars[1]
    for shift, block in zip(shifts, blocks):
        chip = lax.rem(scalars[2] + shift + zs, zs)
        block[pl.ds(core * pairs, pairs)] = own[chip]
        block[pl.ds((1 - core) * pairs, pairs)] = theirs[chip]


def cut_kernel(shifts, zs, scalars, whole, *blocks):
    for shift, block in zip(shifts, blocks):
        block[...] = whole[lax.rem(scalars[2] + shift + zs, zs)]


def split_kernel(shifts, zs, scalars, *refs):
    blocks, (mine, theirs) = refs[:-2], refs[-2:]
    pairs = mine.shape[1]
    core = scalars[1]
    for shift, block in zip(shifts, blocks):
        chip = lax.rem(scalars[2] - shift + zs, zs)
        mine[chip] = block[pl.ds(core * pairs, pairs)]
        theirs[chip] = block[pl.ds((1 - core) * pairs, pairs)]


def gather_kernel(shifts, zs, scalars, *refs):
    blocks, whole = refs[:-1], refs[-1]
    for shift, block in zip(shifts, blocks):
        whole[lax.rem(scalars[2] - shift + zs, zs)] = block[...]


def move(kernel, scalars, arrays, shapes, mib):
    shifts = (0,) + FAR_FIRST
    return pl.pallas_call(
        functools.partial(kernel, shifts, lax.axis_size("z")),
        in_specs=[pl.BlockSpec(memory_space=pltpu.SMEM)] + [VMEM] * len(arrays),
        out_specs=[VMEM] * len(shapes),
        out_shape=[pltpu.VMEM(shape, BF16) for shape in shapes],
        compiler_params=grant(mib),
    )(scalars, *arrays)


def other_core(x):
    return lax.ppermute(x, "core", [(0, 1), (1, 0)])


def send_over_z(blocks):
    n = lax.axis_size("z")
    arrived = []
    for shift, block in zip(FAR_FIRST, blocks):
        pairs = [(i, (i + shift) % n) for i in range(n)]
        arrived.append(lax.ppermute(block, "z", pairs))
    return arrived


def body(left_ops, rotation, integrals, right_ops, states, sector_sizes, couplings, pair_order):
    core = lax.axis_index("core")
    zs = lax.axis_size("z")
    cores = lax.axis_size("core")
    me = lax.axis_index("z")
    width = rotation.shape[2]
    pairs = left_ops.shape[1]
    roots, rows = states.shape[1], states.shape[2]
    sectors = lax.axis_size(SEC)
    all_pairs = integrals.shape[1]

    left = pltpu.with_memory_space_constraint(left_ops[0], pltpu.HBM)
    turn = pltpu.with_memory_space_constraint(rotation[0], pltpu.HBM)
    place = jnp.stack([sector_sizes[0], core.astype(jnp.int32), me.astype(jnp.int32)])
    own, other = rotate(left, turn, place, zs, rows, 11)
    theirs = other_core(other)

    copies = jnp.broadcast_to(states, (sectors, *states.shape[1:]))
    sources = lax.all_to_all(copies, SEC, 0, 0, tiled=True)

    message = (cores * pairs, rows, width)
    blocks = move(join_kernel, place, (own, theirs), [message] * zs, 4)
    arrived = send_over_z(blocks[1:])
    arrived = [pltpu.with_memory_space_constraint(block, pltpu.VMEM) for block in arrived]
    (rotated_all,) = move(gather_kernel, place, [blocks[0]] + arrived, [(zs, *message)], 4)
    rotated_all = rotated_all.reshape(all_pairs, rows, width)

    taken = (jnp.arange(all_pairs, dtype=jnp.int32)[:, None] == pair_order[None, :]).astype(BF16)
    ordered = jnp.dot(integrals, taken, preferred_element_type=F32).astype(BF16)
    ordered, rotated_all = lax.optimization_barrier((ordered, rotated_all))

    sector_ids = jnp.arange(sectors, dtype=jnp.int32)
    weights = jnp.sum((couplings[0][:, None] == sector_ids[None, :]).astype(F32), axis=0)
    mixed_rows = jnp.sum(weights[:, None, None, None] * sources.astype(F32), axis=0).astype(BF16)
    copies = jnp.broadcast_to(mixed_rows[None], (zs, *mixed_rows.shape))
    mixed_z = lax.all_to_all(copies, "z", 0, 0, tiled=True)
    mixed_other = other_core(mixed_z)
    image = make_image(place, mixed_z, mixed_other, right_ops[0])

    comp = jnp.einsum("qi,iab->qab", ordered, rotated_all, preferred_element_type=F32)
    comp = comp.astype(BF16)
    comp = comp.reshape(zs, cores * pairs, rows, width)

    blocks = move(cut_kernel, place, (comp,), [message] * zs, 4)
    arrived = send_over_z(blocks[1:])
    arrived = [pltpu.with_memory_space_constraint(block, pltpu.VMEM) for block in arrived]
    half = (zs, pairs, rows, width)
    mine, theirs = move(split_kernel, place, [blocks[0]] + arrived, [half] * 2, 4)
    theirs = other_core(theirs)
    total, given = make_sigma(mine, theirs, image)
    theirs = other_core(given)
    parts = (total + theirs.astype(F32)).astype(BF16).reshape(zs, rows, roots * width)
    parts = lax.all_to_all(parts, "z", 0, 0, tiled=True)
    result = parts.astype(F32).sum(axis=0)
    return result.reshape(rows, roots, width).transpose(1, 0, 2)[None]


def solution(mesh):
    torus = Mesh(mesh.devices.reshape(4, 4, -1, 2), ("y", "x", "z", "core"))
    placed = (
        P(SEC, PAIR, None, None),
        P(SEC, None, None),
        P(),
        P(SEC, PAIR, None, None),
        P(SEC, None, PAIR, None),
        P(SEC),
        P(SEC, None),
        P(),
    )
    return jax.shard_map(
        body, mesh=torus, in_specs=placed, out_specs=P(SEC, None, PAIR, None), check_vma=False
    )
```

```python
import functools

import jax
import jax.numpy as jnp
from jax import lax
from jax.experimental import pallas as pl
from jax.experimental.pallas import tpu as pltpu
from jax.sharding import Mesh
from jax.sharding import PartitionSpec as P


SEC = ("y", "x")
PAIR = ("z", "core")
FAR_FIRST = (4, 3, -3, 2, -2, -1, 1)
F32 = jnp.float32
BF16 = jnp.bfloat16
VMEM = pl.BlockSpec(memory_space=pltpu.VMEM)


def grant(mib):
    return pltpu.CompilerParams(vmem_limit_bytes=mib * 1024 * 1024)


def dot(a, b, dims):
    return lax.dot_general(a, b, (dims, ((), ())), preferred_element_type=F32)


def rotate_kernel(group, zs, rows, scalars, left_hbm, turn_hbm, own, other, left, turn, sems):
    pairs, depth, _ = left.shape
    width = turn.shape[1]
    steps = pairs // group
    first = pltpu.make_async_copy(turn_hbm, turn, sems.at[steps])
    first.start()
    copies = []
    for step in range(steps):
        span = pl.ds(step * group, group)
        copies.append(pltpu.make_async_copy(left_hbm.at[span], left.at[span], sems.at[step]))
        copies[-1].start()
    size, core = scalars[0], scalars[1]
    slot = lax.broadcasted_iota(jnp.int32, (width, width), 0)
    target = lax.broadcasted_iota(jnp.int32, (width, width), 1)
    which = (slot >= zs * rows).astype(jnp.int32)
    rest = slot - which * (zs * rows)
    spot = core + which - 2 * core * which
    chip = lax.shift_right_logical(rest, 3)
    column = chip * (2 * rows) + spot * rows + (rest - chip * rows)
    pick = jnp.where(column == target, 1.0, 0.0).astype(BF16)
    live = lax.broadcasted_iota(jnp.int32, (depth, width), 1) < size
    first.wait()
    kept = jnp.where(live, turn[...].astype(F32), 0.0).astype(BF16)
    mine = dot(pick, kept, ((1,), (1,))).astype(BF16)
    for step in range(steps):
        copies[step].wait()
        base = step * group
        parts = [dot(mine, left[base + g], ((1,), (0,))).astype(BF16) for g in range(group)]
        whole = dot(jnp.concatenate(parts, axis=0), kept, ((1,), (0,))).astype(BF16)
        for g in range(group):
            result = whole[g * width : (g + 1) * width].reshape(2, zs, rows, width)
            own[:, base + g] = result[0]
            other[:, base + g] = result[1]


def rotate(left, turn, scalars, zs, rows, group):
    pairs, depth, _ = left.shape
    width = turn.shape[1]
    shape = pltpu.VMEM((zs, pairs, rows, width), BF16)
    far = pl.BlockSpec(memory_space=pltpu.HBM)
    return pl.pallas_call(
        functools.partial(rotate_kernel, group, zs, rows),
        in_specs=[pl.BlockSpec(memory_space=pltpu.SMEM), far, far],
        out_specs=[VMEM, VMEM],
        out_shape=[shape, shape],
        scratch_shapes=[
            pltpu.VMEM((pairs, depth, depth), BF16),
            pltpu.VMEM((depth, width), BF16),
            pltpu.SemaphoreType.DMA((pairs // group + 1,)),
        ],
        compiler_params=grant(12),
    )(scalars, left, turn)


def image_kernel(chunk, scalars, mine, theirs, right, image, placed, mixed):
    zs, roots, _, width = mine.shape
    pairs = right.shape[0]
    core = scalars[1]
    for chip in range(zs):
        placed[:, chip, core] = mine[chip]
        placed[:, chip, 1 - core] = theirs[chip]
    for root in range(roots):
        mixed[root] = placed[root].reshape(width, width)

    def put(first, count):
        ops = right[pl.ds(first, count)].reshape(count * width, width)
        for start in range(0, roots, chunk):
            block = mixed[start : start + chunk].reshape(chunk * width, width)
            result = dot(block, ops, ((1,), (1,))).astype(BF16)
            for r in range(chunk):
                for j in range(count):
                    image[
                        pl.ds(pl.multiple_of((first + j) * width, width), width),
                        (start + r) * width : (start + r + 1) * width,
                    ] = result[r * width : (r + 1) * width, j * width : (j + 1) * width]

    def step(i, carry):
        put(4 * i, 2)
        put(4 * i + 2, 2)
        return carry

    lax.fori_loop(0, pairs // 4, step, 0)
    for first in range(pairs - pairs % 4, pairs):
        put(first, 1)


def make_image(scalars, mine, theirs, right):
    zs, roots, rows, width = mine.shape
    pairs = right.shape[0]
    return pl.pallas_call(
        functools.partial(image_kernel, 4),
        in_specs=[pl.BlockSpec(memory_space=pltpu.SMEM), VMEM, VMEM, VMEM],
        out_specs=VMEM,
        out_shape=pltpu.VMEM((pairs * width, roots * width), BF16),
        scratch_shapes=[
            pltpu.VMEM((roots, zs, width // (zs * rows), rows, width), BF16),
            pltpu.VMEM((roots, width, width), BF16),
        ],
        compiler_params=grant(6),
    )(scalars, mine, theirs, right)


def sigma_kernel(shifts, scalars, mine_a, mine_b, theirs_a, theirs_b, image, own, other):
    _, pairs, rows, width = mine_a.shape
    zs = len(shifts)
    comp = []
    for q in range(pairs):
        pieces = [part[:, q].reshape(-1, width) for part in (mine_a, mine_b, theirs_a, theirs_b)]
        comp.append(jnp.concatenate(pieces, axis=0))
    sums = jnp.zeros((2 * zs * rows, image.shape[1]), F32)
    for q in range(0, pairs - 1, 2):
        two = jnp.concatenate([comp[q], comp[q + 1]], axis=1)
        sums += dot(two, image[q * width : (q + 2) * width], ((1,), (0,)))
    if pairs % 2:
        sums += dot(comp[pairs - 1], image[(pairs - 1) * width : pairs * width], ((1,), (0,)))
    for slot, shift in enumerate(shifts):
        chip = lax.rem(scalars[2] - shift + zs, zs)
        own[chip] = sums[slot * rows : (slot + 1) * rows]
        low = (zs + slot) * rows
        other[chip] = sums[low : low + rows].astype(BF16)


def make_sigma(scalars, parts, image):
    rows = parts[0].shape[2]
    shifts = (0,) + FAR_FIRST
    shape = (len(shifts), rows, image.shape[1])
    return pl.pallas_call(
        functools.partial(sigma_kernel, shifts),
        in_specs=[pl.BlockSpec(memory_space=pltpu.SMEM)] + [VMEM] * 5,
        out_specs=[VMEM, VMEM],
        out_shape=[pltpu.VMEM(shape, F32), pltpu.VMEM(shape, BF16)],
        compiler_params=grant(8),
    )(scalars, *parts, image)


def join_kernel(shifts, zs, scalars, own, theirs, *blocks):
    pairs = own.shape[1]
    core = scalars[1]
    for shift, block in zip(shifts, blocks):
        chip = lax.rem(scalars[2] + shift + zs, zs)
        block[pl.ds(core * pairs, pairs)] = own[chip]
        block[pl.ds((1 - core) * pairs, pairs)] = theirs[chip]


def cut_kernel(shifts, zs, scalars, whole, *blocks):
    for shift, block in zip(shifts, blocks):
        block[...] = whole[lax.rem(scalars[2] + shift + zs, zs)]


def split_kernel(shifts, zs, scalars, *refs):
    blocks, (mine, theirs) = refs[:-2], refs[-2:]
    pairs = mine.shape[1]
    core = scalars[1]
    for slot, block in enumerate(blocks):
        mine[slot] = block[pl.ds(core * pairs, pairs)]
        theirs[slot] = block[pl.ds((1 - core) * pairs, pairs)]


def gather_kernel(shifts, zs, scalars, *refs):
    blocks, whole = refs[:-1], refs[-1]
    for shift, block in zip(shifts, blocks):
        whole[lax.rem(scalars[2] - shift + zs, zs)] = block[...]


def move(kernel, scalars, arrays, shapes, mib):
    shifts = (0,) + FAR_FIRST
    return pl.pallas_call(
        functools.partial(kernel, shifts, lax.axis_size("z")),
        in_specs=[pl.BlockSpec(memory_space=pltpu.SMEM)] + [VMEM] * len(arrays),
        out_specs=[VMEM] * len(shapes),
        out_shape=[pltpu.VMEM(shape, BF16) for shape in shapes],
        compiler_params=grant(mib),
    )(scalars, *arrays)


def other_core(x):
    return lax.ppermute(x, "core", [(0, 1), (1, 0)])


def send_over_z(blocks):
    n = lax.axis_size("z")
    arrived = []
    for shift, block in zip(FAR_FIRST, blocks):
        pairs = [(i, (i + shift) % n) for i in range(n)]
        arrived.append(lax.ppermute(block, "z", pairs))
    return arrived


def body(left_ops, rotation, integrals, right_ops, states, sector_sizes, couplings, pair_order):
    core = lax.axis_index("core")
    zs = lax.axis_size("z")
    cores = lax.axis_size("core")
    me = lax.axis_index("z")
    width = rotation.shape[2]
    pairs = left_ops.shape[1]
    roots, rows = states.shape[1], states.shape[2]
    sectors = lax.axis_size(SEC)
    all_pairs = integrals.shape[1]

    left = pltpu.with_memory_space_constraint(left_ops[0], pltpu.HBM)
    turn = pltpu.with_memory_space_constraint(rotation[0], pltpu.HBM)
    place = jnp.stack([sector_sizes[0], core.astype(jnp.int32), me.astype(jnp.int32)])
    own, other = rotate(left, turn, place, zs, rows, 11)
    theirs = other_core(other)

    copies = jnp.broadcast_to(states, (sectors, *states.shape[1:]))
    sources = lax.all_to_all(copies, SEC, 0, 0, tiled=True)

    message = (cores * pairs, rows, width)
    blocks = move(join_kernel, place, (own, theirs), [message] * zs, 4)
    arrived = send_over_z(blocks[1:])
    arrived = [pltpu.with_memory_space_constraint(block, pltpu.VMEM) for block in arrived]
    (rotated_all,) = move(gather_kernel, place, [blocks[0]] + arrived, [(zs, *message)], 4)
    rotated_all = rotated_all.reshape(all_pairs, rows, width)

    taken = (jnp.arange(all_pairs, dtype=jnp.int32)[:, None] == pair_order[None, :]).astype(BF16)
    ordered = jnp.dot(integrals, taken, preferred_element_type=F32).astype(BF16)
    ordered, rotated_all = lax.optimization_barrier((ordered, rotated_all))

    sector_ids = jnp.arange(sectors, dtype=jnp.int32)
    weights = jnp.sum((couplings[0][:, None] == sector_ids[None, :]).astype(F32), axis=0)
    mixed_rows = jnp.sum(weights[:, None, None, None] * sources.astype(F32), axis=0).astype(BF16)
    copies = jnp.broadcast_to(mixed_rows[None], (zs, *mixed_rows.shape))
    mixed_z = lax.all_to_all(copies, "z", 0, 0, tiled=True)
    mixed_other = other_core(mixed_z)
    image = make_image(place, mixed_z, mixed_other, right_ops[0])

    comp = jnp.einsum("qi,iab->qab", ordered, rotated_all, preferred_element_type=F32)
    comp = comp.astype(BF16)
    comp = comp.reshape(zs, cores * pairs, rows, width)

    blocks = move(cut_kernel, place, (comp,), [message] * zs, 4)
    arrived = send_over_z(blocks[1:])
    arrived = [pltpu.with_memory_space_constraint(block, pltpu.VMEM) for block in arrived]
    blocks = [blocks[0]] + arrived
    shape = (zs - 2, pairs, rows, width)
    mine_a, theirs_a = move(split_kernel, place, blocks[:-2], [shape] * 2, 4)
    theirs_a = other_core(theirs_a)
    shape = (2, pairs, rows, width)
    mine_b, theirs_b = move(split_kernel, place, blocks[-2:], [shape] * 2, 4)
    theirs_b = other_core(theirs_b)

    total, given = make_sigma(place, (mine_a, mine_b, theirs_a, theirs_b), image)
    theirs = other_core(given)
    parts = (total + theirs.astype(F32)).astype(BF16)
    parts = lax.all_to_all(parts, "z", 0, 0, tiled=True)
    result = parts.astype(F32).sum(axis=0)
    return result.reshape(rows, roots, width).transpose(1, 0, 2)[None]


def solution(mesh):
    torus = Mesh(mesh.devices.reshape(4, 4, -1, 2), ("y", "x", "z", "core"))
    placed = (
        P(SEC, PAIR, None, None),
        P(SEC, None, None),
        P(),
        P(SEC, PAIR, None, None),
        P(SEC, None, PAIR, None),
        P(SEC),
        P(SEC, None),
        P(),
    )
    return jax.shard_map(
        body, mesh=torus, in_specs=placed, out_specs=P(SEC, None, PAIR, None), check_vma=False
    )
```
